32 devices in a mesh: rows: 8 (over y, x, core), cores: 4 (over z).
Axes of the slice: x: 2, y: 2, z: 4, core: 2. Of those that a mesh axis runs over, the one named last changes fastest.
Arguments:
- rhs: float32 [131072, 128], P(('rows', 'cores')), may hold values from -6 to 6
- guess: float32 [131072, 128], P(('rows', 'cores')), may hold values from -4 to 4
- degree: float32 [131072], P(('rows', 'cores')), may hold values from 2 to 6
- weights: bfloat16 [1024, 16, 128, 128], P(('rows', 'cores')), may hold values from -0.1875 to 0.1875
- columns: int32 [1024, 16], P(('rows', 'cores')), may hold values from 0 to 95, as said below
- block_counts: int32 [1024], P(('rows', 'cores')), may hold values from 8 to 16, as said below
- send_lists: int32 [32, 32, 2], P(('rows', 'cores')), may hold values from 0 to 31
- aggregates: int32 [131072], P(('rows', 'cores')), may hold values from 0 to 16383
- coarse_diag: float32 [16384], replicated, may hold values from 4 to 32
Outputs:
- smoothed: float32 [131072, 128], P(('rows', 'cores'))
The draws below stay inside these ranges and needn't reach their ends.
Inputs may be any that keep to these rules, and one draw needn't show every extreme that they name: `block_counts`: every block row has 8 or 16 live slots, and the rows of one device have exactly 320 live slots in all. `columns`: on every device, each table index from 32 up is named by at least one live slot.
All inputs are finite; a program needn't handle non-finite values.
Results may differ from the reference program's by a relative error of at most 0.0022.
Values may be sent and summed in bfloat16 or wider, within the bound.
A program may use at most 128 MiB of HBM per device.

```python
import math
import jax
import jax.numpy as jnp
from jax import lax

NB_DEV = 32
BLOCK = 128
SLOTS = 16
MAXB = 2
RHS = 128
NC = 16384
NBLK = 1024
NV = 131072
DEVICES = 32


def counts_table(key):
    base = jax.random.fold_in(key, 11)
    keys = jax.random.split(base, DEVICES)
    perms = jax.vmap(lambda single: jax.random.permutation(single, NB_DEV))(keys)
    hubby = perms < NB_DEV // 4
    return jnp.where(hubby, SLOTS, SLOTS // 2).astype(jnp.int32)


def draw_block_counts(key, part):
    return counts_table(key).reshape(-1)


def draw_columns(key, part):
    counts = counts_table(key)
    live = (jnp.arange(SLOTS, dtype=jnp.int32)[None, None, :] < counts[:, :, None]).reshape(DEVICES, -1).astype(jnp.int32)
    ranks = jnp.cumsum(live, axis=1) - 1
    remote = DEVICES * MAXB
    livecount = NB_DEV * SLOTS * 5 // 8
    keys = jax.random.split(jax.random.fold_in(key, 23), DEVICES)
    perms = jax.vmap(lambda single: jax.random.permutation(single, livecount))(keys).astype(jnp.int32)
    assigned = jnp.take_along_axis(perms, jnp.clip(ranks, 0, livecount - 1), axis=1)
    filler = jax.random.randint(jax.random.fold_in(key, 31), live.shape, 0, NB_DEV + remote)
    chosen = jnp.where((live == 1) & (assigned < remote), NB_DEV + assigned, filler)
    return chosen.reshape(NB_DEV * DEVICES, SLOTS).astype(jnp.int32)


def draw_aggregates(key, part):
    total = NB_DEV * DEVICES * BLOCK
    per_owner = NC // DEVICES
    device = jnp.arange(total, dtype=jnp.int32) // (NB_DEV * BLOCK)
    inside = jax.random.randint(jax.random.fold_in(key, 41), (total,), 0, per_owner)
    anywhere = jax.random.randint(jax.random.fold_in(key, 47), (total,), 0, NC)
    across = jax.random.randint(jax.random.fold_in(key, 43), (total,), 0, 2) == 0
    own = device * per_owner + inside
    return jnp.where(across, anywhere, own).astype(jnp.int32)


def touch_ends(drawn, rng, low, top_value):
    dims = drawn.shape
    index_at = [jax.random.randint(jax.random.fold_in(rng, axis), (), 0, dims[axis]) for axis in range(len(dims))]
    drawn = drawn.at[tuple(index_at)].set(low)
    longest = dims.index(max(dims))
    index_at[longest] = (index_at[longest] + 1) % dims[longest]
    return drawn.at[tuple(index_at)].set(top_value)


def block_levels(rng, shape, shards, least, high):
    def one(axis_at, shards_of):
        steps = jax.random.uniform(jax.random.fold_in(jax.random.fold_in(rng, 6), axis_at), (shards_of,), jnp.float32, least / len(shards), high / len(shards))
        return jnp.repeat(jnp.exp(steps), shape[axis_at] // shards_of).reshape((-1,) + (1,) * (len(shape) - axis_at - 1))

    loudness = one(*shards[0])
    for cut in shards[1:]:
        loudness = loudness * one(*cut)
    return loudness


def bell_draw(own_key, shape, deviation, bound, shards=(), held_as=jnp.bfloat16):
    level = block_levels(own_key, shape, shards, -0.22, 0.18) if shards else 1.0
    drawn = jax.random.normal(own_key, shape, jnp.float32) * deviation * level
    return jnp.minimum(jnp.maximum(drawn, -bound), bound).astype(held_as)


def setup_inputs(seed: int = 0) -> dict:
    key_of = jax.random.split(jax.random.key(seed), 10)
    return {
        "rhs": bell_draw(key_of[0], (NV, RHS), 1.0, 6.0, ((0, 32),), jnp.float32),
        "guess": bell_draw(key_of[1], (NV, RHS), 0.5, 4.0, ((0, 32),), jnp.float32),
        "degree": jnp.clip(jnp.exp(math.log(6.0) - 1.0986123 * jax.random.uniform(key_of[2], (NV,), jnp.float32) ** block_levels(key_of[2], (NV,), ((0, 32),), -0.2, 0.2)), 2.0, 6.0),
        "weights": bell_draw(key_of[3], (NBLK, SLOTS, BLOCK, BLOCK), (BLOCK * 8) ** -0.5, 0.1875, ((0, 32),)),
        "columns": draw_columns(jax.random.fold_in(key_of[9], 71), 0),
        "block_counts": draw_block_counts(jax.random.fold_in(key_of[9], 71), 0),
        "send_lists": touch_ends(jax.random.randint(key_of[6], (DEVICES, DEVICES, MAXB), 0, NB_DEV), jax.random.fold_in(key_of[6], 1), 0, NB_DEV - 1).astype(jnp.int32),
        "aggregates": draw_aggregates(jax.random.fold_in(key_of[9], 71), 0),
        "coarse_diag": jnp.clip(jnp.exp(jax.random.uniform(key_of[8], (NC,), jnp.float32, math.log(4.0), math.log(32.0))), 4.0, 32.0),
    }


damping = 0.7


def reference(rhs, guess, degree, weights, columns, block_counts, send_lists, aggregates, coarse_diag):
    nblk = weights.shape[0]
    live = (jnp.arange(SLOTS, dtype=jnp.int32)[None, :] < block_counts[:, None]).astype(jnp.bfloat16)
    live_weights = weights * live[:, :, None, None]

    def apply(field):
        blocks = field.astype(jnp.bfloat16).reshape(nblk, BLOCK, RHS)

        def one(device):
            local = lax.dynamic_slice_in_dim(blocks, device * NB_DEV, NB_DEV, 0)
            owners = jnp.arange(DEVICES, dtype=jnp.int32)[:, None] * NB_DEV
            wanted = (owners + send_lists[:, device, :]).reshape(-1).astype(jnp.int32)
            table = jnp.concatenate([local, blocks[wanted]], 0)
            wpart = lax.dynamic_slice_in_dim(live_weights, device * NB_DEV, NB_DEV, 0)
            cpart = lax.dynamic_slice_in_dim(columns, device * NB_DEV, NB_DEV, 0)
            return jnp.einsum('bsij,bsjr->bir', wpart.astype(jnp.float32), table[cpart].astype(jnp.float32))

        offsum = lax.map(one, jnp.arange(DEVICES, dtype=jnp.int32)).reshape(-1, RHS)
        return degree[:, None] * field - offsum

    first = guess + damping * (rhs - apply(guess)) / degree[:, None]
    residue = rhs - apply(first)
    coarse = jax.ops.segment_sum(residue, aggregates, num_segments=NC)
    correction = (coarse / coarse_diag[:, None]).astype(jnp.bfloat16)
    second = first + correction[aggregates].astype(jnp.float32)
    return second + damping * (rhs - apply(second)) / degree[:, None]
```

```python
import functools
import jax
import jax.numpy as jnp
from jax import lax
from jax.experimental import pallas as pl
from jax.experimental.pallas import tpu as pltpu
from jax.sharding import PartitionSpec as P

damping = 0.7
LIMIT = 64 * 1024 * 1024 - 65536
MESH = pl.DeviceIdType.MESH
VM = pl.BlockSpec(memory_space=pltpu.VMEM)
SM = pl.BlockSpec(memory_space=pltpu.SMEM)
ANY = pl.BlockSpec(memory_space=pl.ANY)
f32, bf16, i32 = jnp.float32, jnp.bfloat16, jnp.int32


def column_of(deg, b):
    row = deg[pl.ds(b, 1), :]
    return jnp.transpose(jnp.broadcast_to(row, (row.shape[1], row.shape[1])))


def half_product(w, tab, cols, b, first, count):
    left = jnp.concatenate([w[b, first + s] for s in range(count)], axis=1)
    right = jnp.concatenate([tab[cols[b, first + s]] for s in range(count)], axis=0)
    return jnp.dot(left, right, preferred_element_type=f32)


def relax_kernel(nr, nz, guess, rhs, deg, agg, cols, counts, sends, w_hbm,
                 x1, res, tab_out, hagg_out,
                 w, tab1, tab2, pack, aggpack, hagg, dcol,
                 wsem, osem, s1, r1, s2, r2, sa, ra):
    n = nr * nz
    nb, slots = w.shape[0], w.shape[1]
    mb = pack.shape[0] // n
    me = lax.axis_index("rows") * nz + lax.axis_index("cores")
    barrier = pltpu.get_barrier_semaphore()

    def where(t):
        return (t // nz, lax.rem(t, nz))

    @pl.loop(1, n)
    def _(k):
        pl.semaphore_signal(barrier, 1, device_id=where(lax.rem(me + k, n)), device_id_type=MESH)

    weights_copy = pltpu.make_async_copy(w_hbm, w, wsem)
    weights_copy.start()

    @pl.loop(0, n)
    def _(t):
        for j in range(mb):
            b = sends[t * mb + j]
            pack[t * mb + j] = guess[b].astype(bf16)
            aggpack[t, pl.ds(j, 1), :] = agg[pl.ds(b, 1), :]

    pl.semaphore_wait(barrier, n - 1)

    def data_copy(k, tab, ss, rr):
        t = lax.rem(me + k, n)
        return pltpu.make_async_remote_copy(
            src_ref=pack.at[pl.ds(t * mb, mb)], dst_ref=tab.at[pl.ds(nb + me * mb, mb)],
            send_sem=ss.at[k], recv_sem=rr.at[k], device_id=where(t), device_id_type=MESH)

    def agg_copy(k):
        t = lax.rem(me + k, n)
        return pltpu.make_async_remote_copy(
            src_ref=aggpack.at[t], dst_ref=hagg.at[me],
            send_sem=sa.at[k], recv_sem=ra.at[k], device_id=where(t), device_id_type=MESH)

    @pl.loop(1, n)
    def _(k):
        data_copy(k, tab1, s1, r1).start()

    @pl.loop(1, n)
    def _(k):
        agg_copy(k).start()

    hagg[me] = aggpack[me]
    for j in range(mb):
        tab1[nb + me * mb + j] = pack[me * mb + j]

    @pl.loop(0, nb)
    def _(b):
        tab1[b] = guess[b].astype(bf16)
        dcol[b] = column_of(deg, b)

    weights_copy.wait()

    @pl.loop(1, n)
    def _(k):
        data_copy(k, tab1, s1, r1).wait_recv()

    half = slots // 2

    def off(tab, b):
        low = half_product(w, tab, cols, b, 0, half)
        high = half_product(w, tab, cols, b, half, slots - half)
        return low + jnp.where(counts[b] > half, high, 0.0)

    @pl.loop(0, nb)
    def _(b):
        d, g = dcol[b], guess[b]
        first = g + damping * (rhs[b] - (d * g - off(tab1, b))) / d
        x1[b] = first
        tab2[b] = first.astype(bf16)

    @pl.loop(1, n)
    def _(k):
        data_copy(k, tab1, s1, r1).wait_send()
        agg_copy(k).wait()

    @pl.loop(0, n * mb)
    def _(i):
        pack[i] = x1[sends[i]].astype(bf16)

    @pl.loop(1, n)
    def _(k):
        data_copy(k, tab2, s2, r2).start()

    for j in range(mb):
        tab2[nb + me * mb + j] = pack[me * mb + j]
    hagg_out[...] = hagg[...]

    @pl.loop(1, n)
    def _(k):
        data_copy(k, tab2, s2, r2).wait_recv()

    out_copy = pltpu.make_async_copy(tab2, tab_out, osem)
    out_copy.start()

    @pl.loop(0, nb)
    def _(b):
        res[b] = rhs[b] - (dcol[b] * x1[b] - off(tab2, b))

    @pl.loop(1, n)
    def _(k):
        data_copy(k, tab2, s2, r2).wait_send()

    out_copy.wait()


def restrict_kernel(ways, agg, inv, res, out, *accs):
    for acc in accs:
        acc[...] = jnp.zeros_like(acc)
    span = res.shape[0] // ways
    step = 4

    @pl.loop(0, span // step)
    def _(i):
        for u in range(step):
            for q in range(ways):
                v = q * span + i * step + u
                a = agg[v]
                accs[q][pl.ds(a, 1), :] += res[pl.ds(v, 1), :] * inv[a]

    tile = 64

    @pl.loop(0, out.shape[0] // tile)
    def _(i):
        rows = pl.ds(i * tile, tile)
        total = accs[0][rows, :]
        for acc in accs[1:]:
            total = total + acc[rows, :]
        out[rows, :] = total


def coarse_kernel(nr, nz, parts, orders, coarse, out, acc, sbuf, rbuf, corr, ss, rs, sg, rg):
    nc = coarse.shape[0]
    top = nc // 2
    r, z = lax.axis_index("rows"), lax.axis_index("cores")
    barrier = pltpu.get_barrier_semaphore()

    def partner(bit):
        axis, m = bit
        other = 1 - 2 * lax.rem((r if axis == 0 else z) // m, 2)
        return (r + other * m, z) if axis == 0 else (r, z + other * m)

    def mine(bit):
        axis, m = bit
        return lax.rem((r if axis == 0 else z) // m, 2)

    every = orders[0]
    for bit in every:
        pl.semaphore_signal(barrier, 1, device_id=partner(bit), device_id_type=MESH)
    pl.semaphore_wait(barrier, len(every))

    levels, count = len(every), len(parts)
    base = [sum(parts[:p]) for p in range(count)]
    room, at = [], 0
    for s in range(levels):
        row = []
        for p in range(count):
            size = parts[p] >> s
            row.append((at, size))
            at += size
        room.append(row)

    def sized(size):
        tile = 64
        while size % tile:
            tile //= 2
        return tile

    def rows_of(start, tile, i):
        return pl.ds(pl.multiple_of(start + i * tile, 16), tile)

    def hop(s, p):
        at, size = room[s][p]
        return pltpu.make_async_remote_copy(
            src_ref=sbuf.at[pl.ds(at, size)], dst_ref=rbuf.at[pl.ds(at, size)],
            send_sem=ss.at[s * count + p], recv_sem=rs.at[s * count + p],
            device_id=partner(orders[p][s]), device_id_type=MESH)

    place = list(base)
    for s in range(levels):
        for p in range(count):
            bit = mine(orders[p][s])
            at, size = room[s][p]
            tile = sized(size)
            if s == 0:
                keep, give, source = bit * top + base[p], (1 - bit) * top + base[p], coarse
            else:
                old_at, old_size = room[s - 1][p]
                hop(s - 1, p).wait_recv()
                was = place[p]
                keep, give, source = was + bit * size, was + (1 - bit) * size, acc
                held = coarse if s == 1 else acc
                shift = mine(orders[p][0]) * top if s == 1 else 0
                old_tile = sized(old_size)

                @pl.loop(0, old_size // old_tile)
                def _(i):
                    rows = rows_of(was, old_tile, i)
                    acc[rows, :] = held[rows_of(was + shift, old_tile, i), :] + rbuf[
                        rows_of(old_at, old_tile, i), :].astype(f32)

                place[p] = keep

            @pl.loop(0, size // tile)
            def _(i):
                sbuf[rows_of(at, tile, i), :] = source[rows_of(give, tile, i), :].astype(bf16)

            hop(s, p).start()

    def spread(s, p, start):
        size = parts[p] >> s
        rows = pl.ds(pl.multiple_of(start, 16), size)
        return pltpu.make_async_remote_copy(
            src_ref=corr.at[rows], dst_ref=corr.at[rows],
            send_sem=sg.at[s * count + p], recv_sem=rg.at[s * count + p],
            device_id=partner(orders[p][s]), device_id_type=MESH)

    shift = mine(every[0]) * top
    sent = []
    for s in reversed(range(levels)):
        for p in range(count):
            if s == levels - 1:
                hop(s, p).wait_recv()
                at, size = room[s][p]
                tile = sized(size)
                was = place[p]

                @pl.loop(0, size // tile)
                def _(i):
                    corr[rows_of(was + shift, tile, i), :] = (
                        acc[rows_of(was, tile, i), :] + rbuf[rows_of(at, tile, i), :].astype(f32)
                    ).astype(bf16)
            else:
                sent[-count].wait_recv()
                place[p] = place[p] - mine(orders[p][s + 1]) * (parts[p] >> (s + 1))
            copy = spread(s, p, place[p] + shift)
            copy.start()
            sent.append(copy)

    for copy in sent[-count:]:
        copy.wait_recv()
    for copy in sent:
        copy.wait_send()
    for s in range(levels):
        for p in range(count):
            hop(s, p).wait_send()

    @pl.loop(0, nc // 128)
    def _(i):
        rows = pl.ds(i * 128, 128)
        out[rows, :] = corr[rows, :]


def smooth_kernel(corr, agg, hagg, x1tab, x1, rhs, deg, cols, counts, w_hbm, out,
                  w, fine, tab, x2, tmp, wsem):
    nb, slots, size = w.shape[0], w.shape[1], w.shape[2]
    weights_copy = pltpu.make_async_copy(w_hbm, w, wsem)
    weights_copy.start()

    @pl.loop(0, corr.shape[0] // 128)
    def _(i):
        rows = pl.ds(i * 128, 128)
        fine[rows, :] = corr[rows, :].astype(f32)

    step = 32

    def gather(ids, block):
        @pl.loop(0, size // step)
        def _(i):
            for u in range(step):
                v = i * step + u
                tmp[pl.ds(v, 1), :] = fine[pl.ds(ids[block * size + v], 1), :]

    @pl.loop(0, nb)
    def _(b):
        gather(agg, b)
        second = x1[b] + tmp[...]
        x2[b] = second
        tab[b] = second.astype(bf16)

    @pl.loop(0, tab.shape[0] - nb)
    def _(i):
        gather(hagg, i)
        tab[nb + i] = (x1tab[nb + i].astype(f32) + tmp[...]).astype(bf16)

    weights_copy.wait()
    half = slots // 2

    @pl.loop(0, nb)
    def _(b):
        tmp[...] = half_product(w, tab, cols, b, 0, half)

        @pl.when(counts[b] > half)
        def _():
            tmp[...] += half_product(w, tab, cols, b, half, slots - half)

        d, second = column_of(deg, b), x2[b]
        out[b] = second + damping * (rhs[b] - (d * second - tmp[...])) / d


def halve_orders(nr, nz):
    row_bits = [(0, 1 << k) for k in range(1, nr.bit_length() - 1)]
    z_bits = [(1, 1 << k) for k in range(nz.bit_length() - 1)]
    core = [(0, 1)]
    return [core + row_bits + z_bits, core + row_bits[::-1] + z_bits, core + z_bits + row_bits]


def body(nr, nz, rhs, guess, degree, weights, columns, block_counts, send_lists, aggregates, coarse_diag):
    n = nr * nz
    nb, slots, bs = weights.shape[0], weights.shape[1], weights.shape[2]
    width = rhs.shape[1]
    nc = coarse_diag.shape[0]
    mb = send_lists.shape[2]
    nt = nb + n * mb
    dma = pltpu.SemaphoreType.DMA
    rhs3, guess3 = rhs.reshape(nb, bs, width), guess.reshape(nb, bs, width)
    deg2, agg2 = degree.reshape(nb, bs), aggregates.reshape(nb, bs)
    field = jax.ShapeDtypeStruct((nb, bs, width), f32)

    x1, res, x1tab, hagg = pl.pallas_call(
        functools.partial(relax_kernel, nr, nz),
        out_shape=(field, field, jax.ShapeDtypeStruct((nt, bs, width), bf16),
                   jax.ShapeDtypeStruct((n, mb, bs), i32)),
        in_specs=[VM, VM, VM, VM, SM, SM, SM, ANY],
        out_specs=(VM, VM, ANY, VM),
        scratch_shapes=[
            pltpu.VMEM((nb, slots, bs, bs), bf16),
            pltpu.VMEM((nt, bs, width), bf16),
            pltpu.VMEM((nt, bs, width), bf16),
            pltpu.VMEM((n * mb, bs, width), bf16),
            pltpu.VMEM((n, mb, bs), i32),
            pltpu.VMEM((n, mb, bs), i32),
            pltpu.VMEM((nb, bs, width), f32),
            dma, dma, dma((n,)), dma((n,)), dma((n,)), dma((n,)), dma((n,)), dma((n,)),
        ],
        compiler_params=pltpu.CompilerParams(
            collective_id=1, has_side_effects=True, vmem_limit_bytes=LIMIT),
        name="relax",
    )(guess3, rhs3, deg2, agg2, columns, block_counts, send_lists.reshape(-1), weights)

    ways = 4
    local_coarse = pl.pallas_call(
        functools.partial(restrict_kernel, ways),
        out_shape=jax.ShapeDtypeStruct((nc, width), f32),
        in_specs=[SM, SM, VM],
        out_specs=VM,
        scratch_shapes=[pltpu.VMEM((nc, width), f32)] * ways,
        compiler_params=pltpu.CompilerParams(vmem_limit_bytes=LIMIT),
        name="restrict",
    )(aggregates, 1.0 / coarse_diag, res.reshape(nb * bs, width))

    orders = halve_orders(nr, nz)
    top = nc // 2
    unit = 16 * (n // 2)
    units = top // unit
    parts = [(units + 2) // 3 * unit, (units + 1) // 3 * unit, units // 3 * unit]
    levels = len(orders[0])
    moved = sum(size >> s for s in range(levels) for size in parts)
    sems = dma((levels * 3,))
    correction = pl.pallas_call(
        functools.partial(coarse_kernel, nr, nz, parts, orders),
        out_shape=jax.ShapeDtypeStruct((nc, width), bf16),
        in_specs=[VM],
        out_specs=VM,
        scratch_shapes=[
            pltpu.VMEM((top, width), f32),
            pltpu.VMEM((moved, width), bf16),
            pltpu.VMEM((moved, width), bf16),
            pltpu.VMEM((nc, width), bf16),
            sems, sems, sems, sems,
        ],
        compiler_params=pltpu.CompilerParams(
            collective_id=2, has_side_effects=True, vmem_limit_bytes=LIMIT),
        name="coarse",
    )(local_coarse)

    out = pl.pallas_call(
        smooth_kernel,
        out_shape=field,
        in_specs=[VM, SM, SM, VM, VM, VM, VM, SM, SM, ANY],
        out_specs=VM,
        scratch_shapes=[
            pltpu.VMEM((nb, slots, bs, bs), bf16),
            pltpu.VMEM((nc, width), f32),
            pltpu.VMEM((nt, bs, width), bf16),
            pltpu.VMEM((nb, bs, width), f32),
            pltpu.VMEM((bs, width), f32),
            dma,
        ],
        compiler_params=pltpu.CompilerParams(vmem_limit_bytes=LIMIT),
        name="smooth",
    )(correction, aggregates, hagg.reshape(-1), x1tab, x1, rhs3, deg2, columns, block_counts, weights)
    return out.reshape(nb * bs, width)


def solution(mesh):
    both = ("rows", "cores")
    return jax.shard_map(
        functools.partial(body, mesh.shape["rows"], mesh.shape["cores"]),
        mesh=mesh,
        in_specs=(
            P(both, None), P(both, None), P(both), P(both, None, None, None), P(both, None),
            P(both), P(both, None, None), P(both), P(),
        ),
        out_specs=P(both, None),
        check_vma=False,
    )
```

```python
import functools
import jax
import jax.numpy as jnp
from jax import lax
from jax.experimental import pallas as pl
from jax.experimental.pallas import tpu as pltpu
from jax.sharding import PartitionSpec as P

damping = 0.7
LIMIT = 64 * 1024 * 1024 - 65536
MESH = pl.DeviceIdType.MESH
VM = pl.BlockSpec(memory_space=pltpu.VMEM)
SM = pl.BlockSpec(memory_space=pltpu.SMEM)
ANY = pl.BlockSpec(memory_space=pl.ANY)
f32, bf16, i32 = jnp.float32, jnp.bfloat16, jnp.int32


def column_of(deg, b):
    row = deg[pl.ds(b, 1), :]
    return jnp.transpose(jnp.broadcast_to(row, (row.shape[1], row.shape[1])))


def row_product(w, tab, cols, b):
    slots = w.shape[1]
    left = jnp.concatenate([w[b, s] for s in range(slots)], axis=1)
    right = jnp.concatenate([tab[cols[s, b]] for s in range(slots)], axis=0)
    return jnp.dot(left, right, preferred_element_type=f32)


def each_row(count, step, act):
    @pl.loop(0, count // step)
    def _(i):
        for u in range(step):
            act(i * step + u)


def relax_kernel(nr, nz, guess, rhs_hbm, deg, agg, cols, sends, w_hbm,
                 x1, res, tab_out, hagg_out,
                 w, tab1, tab2, pack, aggpack, hagg, dcol, rhs,
                 wsem, bsem, osem, s1, r1, s2, r2, sa, ra):
    n = nr * nz
    nb = w.shape[0]
    mb = pack.shape[0] // n
    me = lax.axis_index("rows") * nz + lax.axis_index("cores")
    barrier = pltpu.get_barrier_semaphore()

    def where(t):
        return (t // nz, lax.rem(t, nz))

    @pl.loop(1, n)
    def _(k):
        pl.semaphore_signal(barrier, 1, device_id=where(lax.rem(me + k, n)), device_id_type=MESH)

    weights_copy = pltpu.make_async_copy(w_hbm, w, wsem)
    rhs_copy = pltpu.make_async_copy(rhs_hbm, rhs, bsem)
    weights_copy.start()
    rhs_copy.start()

    @pl.loop(0, n)
    def _(t):
        for j in range(mb):
            b = sends[j, t]
            pack[t * mb + j] = guess[b].astype(bf16)
            aggpack[t, pl.ds(j, 1), :] = agg[pl.ds(b, 1), :]

    pl.semaphore_wait(barrier, n - 1)

    def data_copy(k, tab, ss, rr):
        t = lax.rem(me + k, n)
        return pltpu.make_async_remote_copy(
            src_ref=pack.at[pl.ds(t * mb, mb)], dst_ref=tab.at[pl.ds(nb + me * mb, mb)],
            send_sem=ss.at[k], recv_sem=rr.at[k], device_id=where(t), device_id_type=MESH)

    def agg_copy(k):
        t = lax.rem(me + k, n)
        return pltpu.make_async_remote_copy(
            src_ref=aggpack.at[t], dst_ref=hagg.at[me],
            send_sem=sa.at[k], recv_sem=ra.at[k], device_id=where(t), device_id_type=MESH)

    @pl.loop(1, n)
    def _(k):
        data_copy(k, tab1, s1, r1).start()

    @pl.loop(1, n)
    def _(k):
        agg_copy(k).start()

    hagg[me] = aggpack[me]
    for j in range(mb):
        tab1[nb + me * mb + j] = pack[me * mb + j]

    @pl.loop(0, nb)
    def _(b):
        tab1[b] = guess[b].astype(bf16)
        dcol[b] = column_of(deg, b)

    for tab in (tab1, tab2):
        tab[nb + n * mb] = jnp.zeros(tab.shape[1:], bf16)
    weights_copy.wait()
    rhs_copy.wait()

    @pl.loop(1, n)
    def _(k):
        data_copy(k, tab1, s1, r1).wait_recv()

    def sweep(b):
        d, g = dcol[b], guess[b]
        first = g + damping * (rhs[b] - (d * g - row_product(w, tab1, cols, b))) / d
        x1[b] = first
        tab2[b] = first.astype(bf16)

    each_row(nb, 4, sweep)

    @pl.loop(1, n)
    def _(k):
        data_copy(k, tab1, s1, r1).wait_send()
        agg_copy(k).wait()

    @pl.loop(0, n)
    def _(t):
        for j in range(mb):
            pack[t * mb + j] = x1[sends[j, t]].astype(bf16)

    @pl.loop(1, n)
    def _(k):
        data_copy(k, tab2, s2, r2).start()

    for j in range(mb):
        tab2[nb + me * mb + j] = pack[me * mb + j]
    hagg_out[...] = hagg[...]

    @pl.loop(1, n)
    def _(k):
        data_copy(k, tab2, s2, r2).wait_recv()

    out_copy = pltpu.make_async_copy(tab2, tab_out, osem)
    out_copy.start()

    def residue(b):
        res[b] = rhs[b] - (dcol[b] * x1[b] - row_product(w, tab2, cols, b))

    each_row(nb, 4, residue)

    @pl.loop(1, n)
    def _(k):
        data_copy(k, tab2, s2, r2).wait_send()

    out_copy.wait()


def restrict_kernel(ways, agg, inv, res, out, *scratch):
    accs, sem = scratch[:ways], scratch[ways]
    for acc in accs:
        acc[...] = jnp.zeros_like(acc)
    span = res.shape[0] // ways
    step = 8

    @pl.loop(0, span // step)
    def _(i):
        for u in range(step):
            places = [agg[q * span + i * step + u] for q in range(ways)]
            sums = [
                accs[q][pl.ds(places[q], 1), :]
                + res[pl.ds(q * span + i * step + u, 1), :] * inv[places[q]]
                for q in range(ways)
            ]
            for q in range(ways):
                accs[q][pl.ds(places[q], 1), :] = sums[q]

    tile, pieces = 64, 8
    piece = out.shape[0] // pieces
    copies = []
    for c in range(pieces):
        @pl.loop(0, piece // tile)
        def _(i):
            rows = pl.ds(c * piece + i * tile, tile)
            total = accs[0][rows, :]
            for acc in accs[1:]:
                total = total + acc[rows, :]
            accs[0][rows, :] = total

        rows = pl.ds(c * piece, piece)
        copy = pltpu.make_async_copy(accs[0].at[rows], out.at[rows], sem.at[c])
        copy.start()
        copies.append(copy)
    for copy in copies:
        copy.wait()


def coarse_kernel(nr, nz, parts, orders, coarse_hbm, out, coarse, acc, sbuf, rbuf, corr, ss, rs, sg, rg, load, store):
    nc = coarse.shape[0]
    top = nc // 2
    r, z = lax.axis_index("rows"), lax.axis_index("cores")
    barrier = pltpu.get_barrier_semaphore()

    def partner(bit):
        axis, m = bit
        other = 1 - 2 * lax.rem((r if axis == 0 else z) // m, 2)
        return (r + other * m, z) if axis == 0 else (r, z + other * m)

    def mine(bit):
        axis, m = bit
        return lax.rem((r if axis == 0 else z) // m, 2)

    every = orders[0]
    count = len(parts)
    base = [sum(parts[:p]) for p in range(count)]
    loads = []
    for side in range(2):
        for p in range(count):
            start = lax.rem(1 - mine(every[0]) + side, 2) * top + base[p]
            rows = pl.ds(pl.multiple_of(start, 16), parts[p])
            copy = pltpu.make_async_copy(coarse_hbm.at[rows], coarse.at[rows], load.at[side * count + p])
            copy.start()
            loads.append(copy)

    for bit in every:
        pl.semaphore_signal(barrier, 1, device_id=partner(bit), device_id_type=MESH)
    pl.semaphore_wait(barrier, len(every))

    levels = len(every)
    room, at = [], 0
    for s in range(levels):
        row = []
        for p in range(count):
            size = parts[p] >> s
            row.append((at, size))
            at += size
        room.append(row)

    def sized(size):
        tile = 64
        while size % tile:
            tile //= 2
        return tile

    def rows_of(start, tile, i):
        return pl.ds(pl.multiple_of(start + i * tile, 16), tile)

    def hop(s, p):
        at, size = room[s][p]
        return pltpu.make_async_remote_copy(
            src_ref=sbuf.at[pl.ds(at, size)], dst_ref=rbuf.at[pl.ds(at, size)],
            send_sem=ss.at[s * count + p], recv_sem=rs.at[s * count + p],
            device_id=partner(orders[p][s]), device_id_type=MESH)

    place = list(base)
    for s in range(levels):
        for p in range(count):
            bit = mine(orders[p][s])
            at, size = room[s][p]
            tile = sized(size)
            if s == 0:
                loads[p].wait()
                keep, give, source = bit * top + base[p], (1 - bit) * top + base[p], coarse
            else:
                old_at, old_size = room[s - 1][p]
                hop(s - 1, p).wait_recv()
                if s == 1:
                    loads[count + p].wait()
                was = place[p]
                keep, give, source = was + bit * size, was + (1 - bit) * size, acc
                held = coarse if s == 1 else acc
                shift = mine(orders[p][0]) * top if s == 1 else 0
                old_tile = sized(old_size)

                @pl.loop(0, old_size // old_tile)
                def _(i):
                    rows = rows_of(was, old_tile, i)
                    acc[rows, :] = held[rows_of(was + shift, old_tile, i), :] + rbuf[
                        rows_of(old_at, old_tile, i), :].astype(f32)

                place[p] = keep

            @pl.loop(0, size // tile)
            def _(i):
                sbuf[rows_of(at, tile, i), :] = source[rows_of(give, tile, i), :].astype(bf16)

            hop(s, p).start()

    def spread(s, p, start):
        size = parts[p] >> s
        rows = pl.ds(pl.multiple_of(start, 16), size)
        return pltpu.make_async_remote_copy(
            src_ref=corr.at[rows], dst_ref=corr.at[rows],
            send_sem=sg.at[s * count + p], recv_sem=rg.at[s * count + p],
            device_id=partner(orders[p][s]), device_id_type=MESH)

    shift = mine(every[0]) * top
    sent = []
    for s in reversed(range(levels)):
        for p in range(count):
            if s == levels - 1:
                hop(s, p).wait_recv()
                at, size = room[s][p]
                tile = sized(size)
                was = place[p]

                @pl.loop(0, size // tile)
                def _(i):
                    corr[rows_of(was + shift, tile, i), :] = (
                        acc[rows_of(was, tile, i), :] + rbuf[rows_of(at, tile, i), :].astype(f32)
                    ).astype(bf16)
            else:
                sent[-count].wait_recv()
                place[p] = place[p] - mine(orders[p][s + 1]) * (parts[p] >> (s + 1))
            copy = spread(s, p, place[p] + shift)
            copy.start()
            sent.append(copy)

    def flush(start, size, index):
        rows = pl.ds(pl.multiple_of(start, 16), size)
        return pltpu.make_async_copy(corr.at[rows], out.at[rows], store.at[index])

    flushes = [flush(shift, top, 0)]
    flushes[0].start()
    for p in range(count):
        sent[p - count].wait_recv()
        flushes.append(flush(top - shift + base[p], parts[p], 1 + p))
        flushes[-1].start()
    for copy in sent:
        copy.wait_send()
    for s in range(levels):
        for p in range(count):
            hop(s, p).wait_send()

    for copy in flushes:
        copy.wait()


def smooth_kernel(corr, agg, hagg, x1tab, x1_hbm, rhs_hbm, deg, cols, w_hbm, out,
                  w, fine, tab, x2, rhs, sems):
    nb, size = w.shape[0], w.shape[2]
    pairs = ((x1tab, tab), (x1_hbm, x2), (w_hbm, w), (rhs_hbm, rhs))
    copies = [pltpu.make_async_copy(a, b, sems.at[k]) for k, (a, b) in enumerate(pairs)]
    for copy in copies:
        copy.start()

    @pl.loop(0, corr.shape[0] // 128)
    def _(i):
        rows = pl.ds(i * 128, 128)
        fine[rows, :] = corr[rows, :].astype(f32)

    copies[0].wait()
    copies[1].wait()
    step = 16

    def gathered(ids, first):
        return jnp.concatenate([fine[pl.ds(ids[first + u], 1), :] for u in range(step)], axis=0)

    @pl.loop(0, nb)
    def _(b):
        for i in range(size // step):
            rows = slice(i * step, (i + 1) * step)
            second = x2[b, rows, :] + gathered(agg, b * size + i * step)
            x2[b, rows, :] = second
            tab[b, rows, :] = second.astype(bf16)

    @pl.loop(nb, tab.shape[0] - 1)
    def _(b):
        for i in range(size // step):
            rows = slice(i * step, (i + 1) * step)
            moved = tab[b, rows, :].astype(f32) + gathered(hagg, (b - nb) * size + i * step)
            tab[b, rows, :] = moved.astype(bf16)

    copies[2].wait()
    copies[3].wait()

    def finish(b):
        d, second = column_of(deg, b), x2[b]
        out[b] = second + damping * (rhs[b] - (d * second - row_product(w, tab, cols, b))) / d

    each_row(nb, 4, finish)


def halve_orders(nr, nz):
    row_bits = [(0, 1 << k) for k in range(1, nr.bit_length() - 1)]
    z_bits = [(1, 1 << k) for k in range(nz.bit_length() - 1)]
    core = [(0, 1)]
    return 2 * [
        core + row_bits[:1] + z_bits[:1] + row_bits[1:] + z_bits[1:],
        core + row_bits[::-1] + z_bits,
        core + z_bits + row_bits,
    ]


def body(nr, nz, rhs, guess, degree, weights, columns, block_counts, send_lists, aggregates, coarse_diag):
    n = nr * nz
    nb, slots, bs = weights.shape[0], weights.shape[1], weights.shape[2]
    width = rhs.shape[1]
    nc = coarse_diag.shape[0]
    mb = send_lists.shape[2]
    nt = nb + n * mb + 1
    dma = pltpu.SemaphoreType.DMA
    rhs3, guess3 = rhs.reshape(nb, bs, width), guess.reshape(nb, bs, width)
    deg2, agg2 = degree.reshape(nb, bs), aggregates.reshape(nb, bs)
    live = jnp.arange(slots, dtype=i32)[:, None] < block_counts[None, :]
    cols = jnp.where(live, columns.T, nt - 1)
    field = jax.ShapeDtypeStruct((nb, bs, width), f32)

    x1, res, x1tab, hagg = pl.pallas_call(
        functools.partial(relax_kernel, nr, nz),
        out_shape=(field, field, jax.ShapeDtypeStruct((nt, bs, width), bf16),
                   jax.ShapeDtypeStruct((n, mb, bs), i32)),
        in_specs=[VM, ANY, VM, VM, SM, SM, ANY],
        out_specs=(VM, VM, ANY, VM),
        scratch_shapes=[
            pltpu.VMEM((nb, slots, bs, bs), bf16),
            pltpu.VMEM((nt, bs, width), bf16),
            pltpu.VMEM((nt, bs, width), bf16),
            pltpu.VMEM((n * mb, bs, width), bf16),
            pltpu.VMEM((n, mb, bs), i32),
            pltpu.VMEM((n, mb, bs), i32),
            pltpu.VMEM((nb, bs, width), f32),
            pltpu.VMEM((nb, bs, width), f32),
            dma, dma, dma, dma((n,)), dma((n,)), dma((n,)), dma((n,)), dma((n,)), dma((n,)),
        ],
        compiler_params=pltpu.CompilerParams(
            collective_id=1, has_side_effects=True, vmem_limit_bytes=LIMIT),
        name="relax",
    )(guess3, rhs3, deg2, agg2, cols, send_lists[0].T, weights)

    ways = 4
    local_coarse = pl.pallas_call(
        functools.partial(restrict_kernel, ways),
        out_shape=jax.ShapeDtypeStruct((nc, width), f32),
        in_specs=[SM, SM, VM],
        out_specs=ANY,
        scratch_shapes=[pltpu.VMEM((nc, width), f32)] * ways + [dma((8,))],
        compiler_params=pltpu.CompilerParams(vmem_limit_bytes=LIMIT),
        name="restrict",
    )(aggregates, 1.0 / coarse_diag, res.reshape(nb * bs, width))

    orders = halve_orders(nr, nz)
    top = nc // 2
    unit = 16 * (n // 2)
    units = top // unit
    count = len(orders)
    parts = [(units + count - 1 - p) // count * unit for p in range(count)]
    levels = len(orders[0])
    moved = sum(size >> s for s in range(levels) for size in parts)
    sems = dma((levels * count,))
    correction = pl.pallas_call(
        functools.partial(coarse_kernel, nr, nz, parts, orders),
        out_shape=jax.ShapeDtypeStruct((nc, width), bf16),
        in_specs=[ANY],
        out_specs=ANY,
        scratch_shapes=[
            pltpu.VMEM((nc, width), f32),
            pltpu.VMEM((top, width), f32),
            pltpu.VMEM((moved, width), bf16),
            pltpu.VMEM((moved, width), bf16),
            pltpu.VMEM((nc, width), bf16),
            sems, sems, sems, sems, dma((2 * count,)), dma((count + 1,)),
        ],
        compiler_params=pltpu.CompilerParams(
            collective_id=2, has_side_effects=True, vmem_limit_bytes=LIMIT),
        name="coarse",
    )(local_coarse)

    out = pl.pallas_call(
        smooth_kernel,
        out_shape=field,
        in_specs=[VM, SM, SM, ANY, ANY, ANY, VM, SM, ANY],
        out_specs=VM,
        scratch_shapes=[
            pltpu.VMEM((nb, slots, bs, bs), bf16),
            pltpu.VMEM((nc, width), f32),
            pltpu.VMEM((nt, bs, width), bf16),
            pltpu.VMEM((nb, bs, width), f32),
            pltpu.VMEM((nb, bs, width), f32),
            dma((4,)),
        ],
        compiler_params=pltpu.CompilerParams(vmem_limit_bytes=LIMIT),
        name="smooth",
    )(correction, aggregates, hagg.reshape(-1), x1tab, x1, rhs3, deg2, cols, weights)
    return out.reshape(nb * bs, width)


def solution(mesh):
    both = ("rows", "cores")
    return jax.shard_map(
        functools.partial(body, mesh.shape["rows"], mesh.shape["cores"]),
        mesh=mesh,
        in_specs=(
            P(both, None), P(both, None), P(both), P(both, None, None, None), P(both, None),
            P(both), P(both, None, None), P(both), P(),
        ),
        out_specs=P(both, None),
        check_vma=False,
    )
```

```python
import functools
import jax
import jax.numpy as jnp
from jax import lax
from jax.experimental import pallas as pl
from jax.experimental.pallas import tpu as pltpu
from jax.sharding import PartitionSpec as P

damping = 0.7
LIMIT = 64 * 1024 * 1024 - 65536
MESH = pl.DeviceIdType.MESH
VM = pl.BlockSpec(memory_space=pltpu.VMEM)
SM = pl.BlockSpec(memory_space=pltpu.SMEM)
ANY = pl.BlockSpec(memory_space=pl.ANY)
f32, bf16, i32 = jnp.float32, jnp.bfloat16, jnp.int32


def column_of(deg, b):
    row = deg[pl.ds(b, 1), :]
    return jnp.transpose(jnp.broadcast_to(row, (row.shape[1], row.shape[1])))


def row_product(w, tab, cols, b):
    slots = w.shape[1]
    left = jnp.concatenate([w[b, s] for s in range(slots)], axis=1)
    right = jnp.concatenate([tab[cols[s, b]] for s in range(slots)], axis=0)
    return jnp.dot(left, right, preferred_element_type=f32)


def each_row(count, step, act):
    @pl.loop(0, count // step)
    def _(i):
        for u in range(step):
            act(i * step + u)


def relax_kernel(nr, nz, guess, rhs_hbm, deg, agg, cols, sends, w_hbm,
                 x1_out, res, tab_out, hagg_out,
                 w, tab1, tab2, pack, aggpack, hagg, dcol, rhs, x1,
                 wsem, bsem, osem, xsem, s1, r1, s2, r2, sa, ra):
    n = nr * nz
    nb = w.shape[0]
    mb = pack.shape[0] // n
    me = lax.axis_index("rows") * nz + lax.axis_index("cores")
    barrier = pltpu.get_barrier_semaphore()

    def where(t):
        return (t // nz, lax.rem(t, nz))

    @pl.loop(1, n)
    def _(k):
        pl.semaphore_signal(barrier, 1, device_id=where(lax.rem(me + k, n)), device_id_type=MESH)

    weights_copy = pltpu.make_async_copy(w_hbm, w, wsem)
    rhs_copy = pltpu.make_async_copy(rhs_hbm, rhs, bsem)
    weights_copy.start()
    rhs_copy.start()

    @pl.loop(0, n)
    def _(t):
        for j in range(mb):
            b = sends[j, t]
            pack[t * mb + j] = guess[b].astype(bf16)
            aggpack[t, pl.ds(j, 1), :] = agg[pl.ds(b, 1), :]

    pl.semaphore_wait(barrier, n - 1)

    def data_copy(k, tab, ss, rr):
        t = lax.rem(me + k, n)
        return pltpu.make_async_remote_copy(
            src_ref=pack.at[pl.ds(t * mb, mb)], dst_ref=tab.at[pl.ds(nb + me * mb, mb)],
            send_sem=ss.at[k], recv_sem=rr.at[k], device_id=where(t), device_id_type=MESH)

    def agg_copy(k):
        t = lax.rem(me + k, n)
        return pltpu.make_async_remote_copy(
            src_ref=aggpack.at[t], dst_ref=hagg.at[me],
            send_sem=sa.at[k], recv_sem=ra.at[k], device_id=where(t), device_id_type=MESH)

    @pl.loop(1, n)
    def _(k):
        data_copy(k, tab1, s1, r1).start()

    @pl.loop(1, n)
    def _(k):
        agg_copy(k).start()

    hagg[me] = aggpack[me]
    for j in range(mb):
        tab1[nb + me * mb + j] = pack[me * mb + j]

    @pl.loop(0, nb)
    def _(b):
        tab1[b] = guess[b].astype(bf16)
        dcol[b] = column_of(deg, b)

    for tab in (tab1, tab2):
        tab[nb + n * mb] = jnp.zeros(tab.shape[1:], bf16)
    weights_copy.wait()
    rhs_copy.wait()

    @pl.loop(1, n)
    def _(k):
        data_copy(k, tab1, s1, r1).wait_recv()

    def sweep(b):
        d, g = dcol[b], guess[b]
        first = g + damping * (rhs[b] - (d * g - row_product(w, tab1, cols, b))) / d
        x1[b] = first
        tab2[b] = first.astype(bf16)

    each_row(nb, 8, sweep)
    x1_copy = pltpu.make_async_copy(x1, x1_out, xsem)
    x1_copy.start()

    @pl.loop(1, n)
    def _(k):
        data_copy(k, tab1, s1, r1).wait_send()
        agg_copy(k).wait()

    @pl.loop(0, n)
    def _(t):
        for j in range(mb):
            pack[t * mb + j] = x1[sends[j, t]].astype(bf16)

    @pl.loop(1, n)
    def _(k):
        data_copy(k, tab2, s2, r2).start()

    for j in range(mb):
        tab2[nb + me * mb + j] = pack[me * mb + j]
    hagg_out[...] = hagg[...]

    @pl.loop(1, n)
    def _(k):
        data_copy(k, tab2, s2, r2).wait_recv()

    out_copy = pltpu.make_async_copy(tab2, tab_out, osem)
    out_copy.start()

    def residue(b):
        res[b] = rhs[b] - (dcol[b] * x1[b] - row_product(w, tab2, cols, b))

    each_row(nb, 8, residue)

    @pl.loop(1, n)
    def _(k):
        data_copy(k, tab2, s2, r2).wait_send()

    out_copy.wait()
    x1_copy.wait()


def restrict_kernel(ways, agg, inv, res, out, *scratch):
    accs, sem = scratch[:ways], scratch[ways]
    for acc in accs:
        acc[...] = jnp.zeros_like(acc)
    span = res.shape[0] // ways
    step = 8

    @pl.loop(0, span // step)
    def _(i):
        for u in range(step):
            places = [agg[q * span + i * step + u] for q in range(ways)]
            sums = [
                accs[q][pl.ds(places[q], 1), :]
                + res[pl.ds(q * span + i * step + u, 1), :] * inv[places[q]]
                for q in range(ways)
            ]
            for q in range(ways):
                accs[q][pl.ds(places[q], 1), :] = sums[q]

    tile, pieces = 64, 8
    piece = out.shape[0] // pieces
    copies = []
    for c in range(pieces):
        @pl.loop(0, piece // tile)
        def _(i):
            rows = pl.ds(c * piece + i * tile, tile)
            total = accs[0][rows, :]
            for acc in accs[1:]:
                total = total + acc[rows, :]
            accs[0][rows, :] = total

        rows = pl.ds(c * piece, piece)
        copy = pltpu.make_async_copy(accs[0].at[rows], out.at[rows], sem.at[c])
        copy.start()
        copies.append(copy)
    for copy in copies:
        copy.wait()


def coarse_kernel(nr, nz, parts, orders, coarse_hbm, out, coarse, acc, sbuf, rbuf, corr, ss, rs, sg, rg, load, store):
    nc = coarse.shape[0]
    top = nc // 2
    r, z = lax.axis_index("rows"), lax.axis_index("cores")
    barrier = pltpu.get_barrier_semaphore()

    def partner(bit):
        axis, m = bit
        other = 1 - 2 * lax.rem((r if axis == 0 else z) // m, 2)
        return (r + other * m, z) if axis == 0 else (r, z + other * m)

    def mine(bit):
        axis, m = bit
        return lax.rem((r if axis == 0 else z) // m, 2)

    every = orders[0]
    count = len(parts)
    base = [sum(parts[:p]) for p in range(count)]
    loads = []
    for side in range(2):
        for p in range(count):
            start = lax.rem(1 - mine(every[0]) + side, 2) * top + base[p]
            rows = pl.ds(pl.multiple_of(start, 16), parts[p])
            copy = pltpu.make_async_copy(coarse_hbm.at[rows], coarse.at[rows], load.at[side * count + p])
            copy.start()
            loads.append(copy)

    for bit in every:
        pl.semaphore_signal(barrier, 1, device_id=partner(bit), device_id_type=MESH)
    pl.semaphore_wait(barrier, len(every))

    levels = len(every)
    room, at = [], 0
    for s in range(levels):
        row = []
        for p in range(count):
            size = parts[p] >> s
            row.append((at, size))
            at += size
        room.append(row)

    def sized(size):
        tile = 64
        while size % tile:
            tile //= 2
        return tile

    def rows_of(start, tile, i):
        return pl.ds(pl.multiple_of(start + i * tile, 16), tile)

    def hop(s, p):
        at, size = room[s][p]
        return pltpu.make_async_remote_copy(
            src_ref=sbuf.at[pl.ds(at, size)], dst_ref=rbuf.at[pl.ds(at, size)],
            send_sem=ss.at[s * count + p], recv_sem=rs.at[s * count + p],
            device_id=partner(orders[p][s]), device_id_type=MESH)

    place = list(base)
    for s in range(levels):
        for p in range(count):
            bit = mine(orders[p][s])
            at, size = room[s][p]
            tile = sized(size)
            if s == 0:
                loads[p].wait()
                keep, give, source = bit * top + base[p], (1 - bit) * top + base[p], coarse
            else:
                old_at, old_size = room[s - 1][p]
                hop(s - 1, p).wait_recv()
                if s == 1:
                    loads[count + p].wait()
                was = place[p]
                keep, give, source = was + bit * size, was + (1 - bit) * size, acc
                held = coarse if s == 1 else acc
                shift = mine(orders[p][0]) * top if s == 1 else 0
                old_tile = sized(old_size)

                @pl.loop(0, old_size // old_tile)
                def _(i):
                    rows = rows_of(was, old_tile, i)
                    acc[rows, :] = held[rows_of(was + shift, old_tile, i), :] + rbuf[
                        rows_of(old_at, old_tile, i), :].astype(f32)

                place[p] = keep

            @pl.loop(0, size // tile)
            def _(i):
                sbuf[rows_of(at, tile, i), :] = source[rows_of(give, tile, i), :].astype(bf16)

            hop(s, p).start()

    def spread(s, p, start):
        size = parts[p] >> s
        rows = pl.ds(pl.multiple_of(start, 16), size)
        return pltpu.make_async_remote_copy(
            src_ref=corr.at[rows], dst_ref=corr.at[rows],
            send_sem=sg.at[s * count + p], recv_sem=rg.at[s * count + p],
            device_id=partner(orders[p][s]), device_id_type=MESH)

    shift = mine(every[0]) * top
    sent = []
    for s in reversed(range(levels)):
        for p in range(count):
            if s == levels - 1:
                hop(s, p).wait_recv()
                at, size = room[s][p]
                tile = sized(size)
                was = place[p]

                @pl.loop(0, size // tile)
                def _(i):
                    corr[rows_of(was + shift, tile, i), :] = (
                        acc[rows_of(was, tile, i), :] + rbuf[rows_of(at, tile, i), :].astype(f32)
                    ).astype(bf16)
            else:
                sent[-count].wait_recv()
                place[p] = place[p] - mine(orders[p][s + 1]) * (parts[p] >> (s + 1))
            copy = spread(s, p, place[p] + shift)
            copy.start()
            sent.append(copy)

    def flush(start, size, index):
        rows = pl.ds(pl.multiple_of(start, 16), size)
        return pltpu.make_async_copy(corr.at[rows], out.at[rows], store.at[index])

    flushes = [flush(shift, top, 0)]
    flushes[0].start()
    for p in range(count):
        sent[p - count].wait_recv()
        flushes.append(flush(top - shift + base[p], parts[p], 1 + p))
        flushes[-1].start()
    for copy in sent:
        copy.wait_send()
    for s in range(levels):
        for p in range(count):
            hop(s, p).wait_send()

    for copy in flushes:
        copy.wait()


def smooth_kernel(corr, agg, hagg, x1tab, x1_hbm, rhs_hbm, deg, cols, w_hbm, out,
                  w, fine, tab, x2, rhs, sems):
    nb, size = w.shape[0], w.shape[2]
    pairs = ((x1tab, tab), (x1_hbm, x2), (w_hbm, w), (rhs_hbm, rhs))
    copies = [pltpu.make_async_copy(a, b, sems.at[k]) for k, (a, b) in enumerate(pairs)]
    for copy in copies:
        copy.start()

    @pl.loop(0, corr.shape[0] // 128)
    def _(i):
        rows = pl.ds(i * 128, 128)
        fine[rows, :] = corr[rows, :].astype(f32)

    copies[0].wait()
    copies[1].wait()
    step = 16

    def gathered(ids, first):
        return jnp.concatenate([fine[pl.ds(ids[first + u], 1), :] for u in range(step)], axis=0)

    @pl.loop(0, nb)
    def _(b):
        for i in range(size // step):
            rows = slice(i * step, (i + 1) * step)
            second = x2[b, rows, :] + gathered(agg, b * size + i * step)
            x2[b, rows, :] = second
            tab[b, rows, :] = second.astype(bf16)

    @pl.loop(nb, tab.shape[0] - 1)
    def _(b):
        for i in range(size // step):
            rows = slice(i * step, (i + 1) * step)
            moved = tab[b, rows, :].astype(f32) + gathered(hagg, (b - nb) * size + i * step)
            tab[b, rows, :] = moved.astype(bf16)

    copies[2].wait()
    copies[3].wait()

    def finish(b):
        d, second = column_of(deg, b), x2[b]
        out[b] = second + damping * (rhs[b] - (d * second - row_product(w, tab, cols, b))) / d

    each_row(nb, 8, finish)


def halve_orders(nr, nz):
    row_bits = [(0, 1 << k) for k in range(1, nr.bit_length() - 1)]
    z_bits = [(1, 1 << k) for k in range(nz.bit_length() - 1)]
    core = [(0, 1)]
    return 2 * [
        core + row_bits[:1] + z_bits[:1] + row_bits[1:] + z_bits[1:],
        core + row_bits[::-1] + z_bits,
        core + z_bits + row_bits,
    ]


def body(nr, nz, rhs, guess, degree, weights, columns, block_counts, send_lists, aggregates, coarse_diag):
    n = nr * nz
    nb, slots, bs = weights.shape[0], weights.shape[1], weights.shape[2]
    width = rhs.shape[1]
    nc = coarse_diag.shape[0]
    mb = send_lists.shape[2]
    nt = nb + n * mb + 1
    dma = pltpu.SemaphoreType.DMA
    rhs3, guess3 = rhs.reshape(nb, bs, width), guess.reshape(nb, bs, width)
    deg2, agg2 = degree.reshape(nb, bs), aggregates.reshape(nb, bs)
    live = jnp.arange(slots, dtype=i32)[:, None] < block_counts[None, :]
    cols = jnp.where(live, columns.T, nt - 1)
    field = jax.ShapeDtypeStruct((nb, bs, width), f32)

    x1, res, x1tab, hagg = pl.pallas_call(
        functools.partial(relax_kernel, nr, nz),
        out_shape=(field, field, jax.ShapeDtypeStruct((nt, bs, width), bf16),
                   jax.ShapeDtypeStruct((n, mb, bs), i32)),
        in_specs=[VM, ANY, VM, VM, SM, SM, ANY],
        out_specs=(ANY, VM, ANY, VM),
        scratch_shapes=[
            pltpu.VMEM((nb, slots, bs, bs), bf16),
            pltpu.VMEM((nt, bs, width), bf16),
            pltpu.VMEM((nt, bs, width), bf16),
            pltpu.VMEM((n * mb, bs, width), bf16),
            pltpu.VMEM((n, mb, bs), i32),
            pltpu.VMEM((n, mb, bs), i32),
            pltpu.VMEM((nb, bs, width), f32),
            pltpu.VMEM((nb, bs, width), f32),
            pltpu.VMEM((nb, bs, width), f32),
            dma, dma, dma, dma, dma((n,)), dma((n,)), dma((n,)), dma((n,)), dma((n,)), dma((n,)),
        ],
        compiler_params=pltpu.CompilerParams(
            collective_id=1, has_side_effects=True, vmem_limit_bytes=LIMIT),
        name="relax",
    )(guess3, rhs3, deg2, agg2, cols, send_lists[0].T, weights)

    ways = 4
    local_coarse = pl.pallas_call(
        functools.partial(restrict_kernel, ways),
        out_shape=jax.ShapeDtypeStruct((nc, width), f32),
        in_specs=[SM, SM, VM],
        out_specs=ANY,
        scratch_shapes=[pltpu.VMEM((nc, width), f32)] * ways + [dma((8,))],
        compiler_params=pltpu.CompilerParams(vmem_limit_bytes=LIMIT),
        name="restrict",
    )(aggregates, 1.0 / coarse_diag, res.reshape(nb * bs, width))

    orders = halve_orders(nr, nz)
    top = nc // 2
    unit = 16 * (n // 2)
    units = top // unit
    count = len(orders)
    parts = [(units + count - 1 - p) // count * unit for p in range(count)]
    levels = len(orders[0])
    moved = sum(size >> s for s in range(levels) for size in parts)
    sems = dma((levels * count,))
    correction = pl.pallas_call(
        functools.partial(coarse_kernel, nr, nz, parts, orders),
        out_shape=jax.ShapeDtypeStruct((nc, width), bf16),
        in_specs=[ANY],
        out_specs=ANY,
        scratch_shapes=[
            pltpu.VMEM((nc, width), f32),
            pltpu.VMEM((top, width), f32),
            pltpu.VMEM((moved, width), bf16),
            pltpu.VMEM((moved, width), bf16),
            pltpu.VMEM((nc, width), bf16),
            sems, sems, sems, sems, dma((2 * count,)), dma((count + 1,)),
        ],
        compiler_params=pltpu.CompilerParams(
            collective_id=2, has_side_effects=True, vmem_limit_bytes=LIMIT),
        name="coarse",
    )(local_coarse)

    out = pl.pallas_call(
        smooth_kernel,
        out_shape=field,
        in_specs=[VM, SM, SM, ANY, ANY, ANY, VM, SM, ANY],
        out_specs=VM,
        scratch_shapes=[
            pltpu.VMEM((nb, slots, bs, bs), bf16),
            pltpu.VMEM((nc, width), f32),
            pltpu.VMEM((nt, bs, width), bf16),
            pltpu.VMEM((nb, bs, width), f32),
            pltpu.VMEM((nb, bs, width), f32),
            dma((4,)),
        ],
        compiler_params=pltpu.CompilerParams(vmem_limit_bytes=LIMIT),
        name="smooth",
    )(correction, aggregates, hagg.reshape(-1), x1tab, x1, rhs3, deg2, cols, weights)
    return out.reshape(nb * bs, width)


def solution(mesh):
    both = ("rows", "cores")
    return jax.shard_map(
        functools.partial(body, mesh.shape["rows"], mesh.shape["cores"]),
        mesh=mesh,
        in_specs=(
            P(both, None), P(both, None), P(both), P(both, None, None, None), P(both, None),
            P(both), P(both, None, None), P(both), P(),
        ),
        out_specs=P(both, None),
        check_vma=False,
    )
```
